32 devices in a mesh: dp: 8 (over z, x), mp: 4 (over y, core).
Axes of the slice: x: 2, y: 2, z: 4, core: 2. Of those that a mesh axis runs over, the one named last changes fastest.
Arguments:
- pool_inputs: bfloat16 [1024, 8, 4096], P('dp', None, 'mp'), may hold values from -6 to 6
- pool_targets: bfloat16 [1024, 8, 4096], P('dp', None, 'mp'), may hold values from -6 to 6
- frozen: bfloat16 [4096, 4096], P(None, 'mp'), may hold values from -0.09375 to 0.09375
- gain: float32 [4096], P('mp'), may hold values from 0.5 to 1.5
- adapter_down: bfloat16 [8, 64, 4096], P('dp', None, 'mp'), may hold values from -0.09375 to 0.09375
- adapter_up: bfloat16 [8, 64, 4096], P('dp', None, 'mp'), may hold values from -0.75 to 0.75
- sample_ids: int32 [512], P('dp'), may hold values from 0 to 127
- buckets: int32 [1024], P('dp'), may hold values from 0 to 15
- lengths: int32 [1024], P('dp'), may hold values from 1 to 8
- destinations: int32 [512, 1], P('dp'), may hold values from 0 to 7; in each aligned block of 64 rows (0 to 63, 64 to 127, ...) at most 12 rows name the same one
- competence: float32 [1], replicated, may hold values from 0.3 to 0.7
Outputs:
- grad_down: float32 [8, 64, 4096], P('dp', None, 'mp')
- grad_up: float32 [8, 64, 4096], P('dp', None, 'mp')
- bucket_loss: float32 [16], replicated
- competence_next: float32 [1], replicated
The draws below stay inside these ranges and needn't reach their ends.
Inputs may be any that keep to these rules, and one draw needn't show every extreme that they name: `destinations`: of the 64 sampled slots of one holder, at most 12 name the same trainer. `sample_ids`: an index into the holder's own 128 stored blocks.
All inputs are finite; a program needn't handle non-finite values.
Results may differ from the reference program's by a relative error of at most 0.0056.
Values may be sent and summed in bfloat16 or wider, within the bound.
A program may use at most 128 MiB of HBM per device.

```python
import math
import jax
import jax.numpy as jnp
import numpy as np
from jax import lax

D = 4096
R = 64
NB = 16
BLK = 8
SEQ_DEV = 64
POOL_DEV = 128
SAMPLED = 512
POOLED = 1024
MOST = 12
N_DP = 8


def with_ends(array, rng, least, high):
    place = [jax.random.randint(jax.random.fold_in(rng, axis), (), 0, length) for axis, length in enumerate(array.shape)]
    widest = array.shape.index(max(array.shape))
    next_to = place[:widest] + [(place[widest] + 1) % array.shape[widest]] + place[widest + 1:]
    return array.at[tuple(place)].set(least).at[tuple(next_to)].set(high)


def steps_of(own_key, shape, split, low, high):
    def one(dim, blocks):
        draws = jax.random.uniform(jax.random.fold_in(jax.random.fold_in(own_key, 6), dim), (blocks,), jnp.float32, low / len(split), high / len(split))
        return jnp.repeat(jnp.exp(draws), shape[dim] // blocks).reshape((-1,) + (1,) * (len(shape) - dim - 1))

    level = one(*split[0])
    for cut in split[1:]:
        level = level * one(*cut)
    return level


def routed_block(rng, own, number, rows, count, top, reach, lean):
    sequence = jax.random.permutation(rng, count)
    heavy_load, common = portions_of(count, rows * top, reach, lean, True), portions_of(count, rows * top, reach, lean, False)
    places = jnp.arange(count)

    def named(sizes, offset_by):
        used = int((sizes > 0).sum())
        fixed = max(1, used // 4)
        shifted = fixed + (places - fixed + offset_by * (used - fixed)) % max(1, count - fixed)
        return jnp.zeros((count,), jnp.int32).at[sequence[jnp.where(places < fixed, places, shifted)]].set(jnp.asarray(sizes, jnp.int32))

    sizes = jnp.where(number % 4 == 0, named(heavy_load, number // 4), named(common, number - number // 4 - 1))
    mixed = jax.random.permutation(jax.random.fold_in(own, 3), count)
    source_of, sink = mixed[0:count // 2 * 2:2], mixed[1:count // 2 * 2:2]
    margin = jnp.minimum(sizes[source_of] - 1, reach - sizes[sink]) // 2
    margin = jnp.where((source_of == sequence[0]) | (sink == sequence[0]) | (sizes[sink] == 0), 0, jnp.maximum(margin, 0))
    shifted = jax.random.randint(jax.random.fold_in(own, 4), (count // 2,), 0, 1 << 20) % (margin + 1)
    sizes = sizes.at[source_of].add(-shifted).at[sink].add(shifted)
    members = jnp.searchsorted(jnp.cumsum(sizes), jnp.arange(rows * top), side="right").astype(jnp.int32)
    listing = members.reshape(top, rows).T
    listing = listing[jax.random.permutation(jax.random.fold_in(own, 1), rows)]
    offset_by = jax.random.randint(jax.random.fold_in(own, 2), (rows, 1), 0, top)
    return jnp.take_along_axis(listing, (jnp.arange(top)[None, :] + offset_by) % top, axis=1)


def portions_of(count, total, bound, lean, full):
    loads = [(1 << 20) // math.isqrt(standing ** lean) + 1 for standing in range(1, count + 1)]
    largest = bound if full else min(bound, max(-(-total // count), total * loads[0] // sum(loads)))
    least = 1 if total - largest >= count - 1 else 0
    holding, spare = [largest] + [least] * (count - 1), total - largest - least * (count - 1)
    while spare > 0:
        candidates = [i for i in range(1, count) if holding[i] < largest] or [i for i in range(1, count) if holding[i] < bound]
        whole, left = sum([loads[i] for i in candidates]), spare
        for i in candidates:
            more = min(bound - holding[i], max(1, left * loads[i] // whole), spare)
            holding[i] = holding[i] + more
            spare = spare - more
    return np.array(holding)


def gaussian(stream_key, extent, width, most, cuts=(), kind=jnp.bfloat16):
    loudness = steps_of(stream_key, extent, cuts, -0.22, 0.18) if cuts else 1.0
    drawn = jax.random.normal(stream_key, extent, jnp.float32) * width * loudness
    return jnp.minimum(jnp.maximum(drawn, -most), most).astype(kind)


def setup_inputs(seed: int = 0) -> dict:
    splits = jax.random.split(jax.random.key(seed), 12)
    pool_inputs = gaussian(splits[0], (POOLED, BLK, D), 1.0, 6.0, ((0, 8), (2, 4)))
    pool_targets = gaussian(splits[1], (POOLED, BLK, D), 1.0, 6.0, ((0, 8), (2, 4)))
    frozen = gaussian(splits[2], (D, D), D ** -0.5, 0.09375, ((1, 4),))
    gain = jnp.clip(1.0 + 0.1 * jax.random.normal(splits[3], (D,), jnp.float32), 0.5, 1.5)
    adapter_down = gaussian(splits[4], (N_DP, R, D), D ** -0.5, 0.09375, ((0, 8), (2, 4)))
    adapter_up = gaussian(splits[5], (N_DP, R, D), R ** -0.5, 0.75, ((0, 8), (2, 4)))
    sample_ids = with_ends(jax.random.randint(splits[6], (SAMPLED,), 0, POOL_DEV), jax.random.fold_in(splits[6], 1), 0, POOL_DEV - 1).astype(jnp.int32)
    buckets = with_ends(jax.random.randint(splits[7], (POOLED,), 0, NB), jax.random.fold_in(splits[7], 1), 0, NB - 1).astype(jnp.int32)
    lengths = with_ends(jax.random.randint(splits[8], (POOLED,), 1, BLK + 1), jax.random.fold_in(splits[8], 1), 1, BLK).astype(jnp.int32)
    destinations_keys = jax.random.split(jax.random.fold_in(splits[9], 1), SAMPLED // SEQ_DEV)
    destinations_turns = jax.random.permutation(jax.random.fold_in(splits[9], 3), SAMPLED // SEQ_DEV)
    destinations = jax.vmap(lambda own, number: routed_block(jax.random.fold_in(splits[9], 2), own, number, SEQ_DEV, N_DP, 1, MOST, 2))(destinations_keys, destinations_turns).reshape((SAMPLED, 1))
    competence = jnp.clip(jax.random.uniform(splits[10], (1,), jnp.float32, 0.3, 0.7), 0.3, 0.7)
    return {"pool_inputs": pool_inputs, "pool_targets": pool_targets, "frozen": frozen, "gain": gain, "adapter_down": adapter_down, "adapter_up": adapter_up, "sample_ids": sample_ids, "buckets": buckets, "lengths": lengths, "destinations": destinations, "competence": competence}


RMS_EPSILON = 1e-05
SHARPNESS = 12.0
ADAPTER_SCALING = 2.0

def normalize(values, gain):
    inverse_rms = lax.rsqrt(lax.optimization_barrier(jnp.mean(values * values, axis=-1, keepdims=True)) + RMS_EPSILON)
    return (values * inverse_rms * gain).astype(jnp.bfloat16)

def reference(pool_inputs, pool_targets, frozen, gain, adapter_down, adapter_up, sample_ids, buckets, lengths, destinations, competence):
    holder = (jnp.arange(SAMPLED) // SEQ_DEV).astype(jnp.int32)
    picked = (holder * POOL_DEV + sample_ids).astype(jnp.int32)
    inputs = jnp.take(pool_inputs, picked, axis=0).reshape(SAMPLED * BLK, D).astype(jnp.float32)
    normed = normalize(inputs, gain)
    targets = jnp.take(pool_targets, picked, axis=0).reshape(SAMPLED * BLK, D).astype(jnp.float32)
    base_gap = (inputs + jnp.dot(normed, frozen, preferred_element_type=jnp.float32) - targets).astype(jnp.bfloat16)
    normed = normed.reshape(SAMPLED, BLK, D)
    base_gap = base_gap.reshape(SAMPLED, BLK, D)
    block_bucket = jnp.take(buckets, picked)
    block_length = jnp.take(lengths, picked)
    bucket_onehot = (block_bucket[:, None] == jnp.arange(NB, dtype=jnp.int32)[None, :]).astype(jnp.float32)
    counts = lax.optimization_barrier(jnp.sum(bucket_onehot * block_length[:, None].astype(jnp.float32), axis=0))
    floor_counts = jnp.maximum(counts, 1.0)
    weights = jax.nn.sigmoid(SHARPNESS * (competence[0] - (jnp.arange(NB).astype(jnp.float32) + 0.5) / NB))
    block_coefficient = lax.optimization_barrier(jnp.sum(bucket_onehot * (weights / floor_counts)[None, :], axis=1))
    target_trainer = destinations[:, 0]
    by_trainer = jnp.argsort(target_trainer, stable=True).astype(jnp.int32)
    per_count = lax.optimization_barrier(jnp.sum((target_trainer[:, None] == jnp.arange(N_DP, dtype=jnp.int32)[None, :]).astype(jnp.int32), axis=0))
    first_block = (jnp.cumsum(per_count) - per_count).astype(jnp.int32)
    block_capacity = N_DP * MOST

    def trainer(trainer_position_index):
        slot_ids = jnp.arange(block_capacity, dtype=jnp.int32)
        occupied = slot_ids < per_count[trainer_position_index]
        block_ids = by_trainer[jnp.minimum(first_block[trainer_position_index] + slot_ids, SAMPLED - 1)]
        normed_rows = normed[block_ids].reshape(block_capacity * BLK, D)
        gap_rows = base_gap[block_ids].reshape(block_capacity * BLK, D).astype(jnp.float32)
        live_lengths = jnp.where(occupied, block_length[block_ids], 0)
        live_mask = (jnp.arange(BLK, dtype=jnp.int32)[None, :] < live_lengths[:, None]).astype(jnp.float32).reshape(-1)
        row_coefficient = jnp.repeat(block_coefficient[block_ids], BLK)
        down_map = adapter_down[trainer_position_index]
        up_map = adapter_up[trainer_position_index]
        latent_rows = jnp.dot(normed_rows, down_map.T, preferred_element_type=jnp.float32)
        lowered_rows = (ADAPTER_SCALING * latent_rows).astype(jnp.bfloat16)
        distance = gap_rows + jnp.dot(lowered_rows, up_map, preferred_element_type=jnp.float32)
        output_grad = ((2.0 * row_coefficient * live_mask)[:, None] * distance).astype(jnp.bfloat16)
        latent_gradient = jnp.dot(output_grad, up_map.T, preferred_element_type=jnp.float32)
        lowered_gradient = (ADAPTER_SCALING * latent_gradient).astype(jnp.bfloat16)
        up_gradient = jnp.dot(lowered_rows.T, output_grad, preferred_element_type=jnp.float32)
        down_gradient = jnp.dot(lowered_gradient.T, normed_rows, preferred_element_type=jnp.float32)
        block_square = lax.optimization_barrier(jnp.sum((lax.optimization_barrier(jnp.sum(distance * distance, axis=1)) * live_mask).reshape(block_capacity, BLK), axis=1))
        slot_onehot = bucket_onehot[block_ids] * occupied[:, None].astype(jnp.float32)
        partial_value = lax.optimization_barrier(jnp.sum(slot_onehot * block_square[:, None], axis=0))
        return (down_gradient, up_gradient, partial_value)
    grad_down, grad_up, partials = lax.map(trainer, jnp.arange(N_DP, dtype=jnp.int32))
    bucket_loss = lax.optimization_barrier(jnp.sum(partials, axis=0)) / (floor_counts * D)
    progress = jnp.sum(weights * bucket_loss) / jnp.sum(bucket_loss)
    competence_next = competence + 0.5 * (1.0 - competence) * progress
    return (grad_down, grad_up, bucket_loss, competence_next)
```

```python
import functools

import jax
import jax.numpy as jnp
from jax import lax
from jax.experimental import pallas as pl
from jax.experimental.pallas import tpu as pltpu
from jax.sharding import PartitionSpec as P

NB = 16


RMS_EPSILON = 1e-05
SHARPNESS = 12.0
ADAPTER_SCALING = 2.0


def normalize(values, gain, model_width):
    partial_value = jnp.sum(values * values, axis=1)
    square_total = lax.psum(partial_value, "mp")
    inverse_rms = lax.rsqrt(square_total / model_width + RMS_EPSILON)
    return (values * inverse_rms[:, None] * gain[None, :]).astype(jnp.bfloat16)


def frozen_gap(values, normed, targets, frozen):
    projected = jnp.dot(
        lax.all_gather(normed, "mp", axis=1, tiled=True), frozen, preferred_element_type=jnp.float32
    )
    return (values + projected - targets.astype(jnp.float32)).astype(jnp.bfloat16)


def place_blocks(placing, sequence_blocks):
    flat_blocks = sequence_blocks.reshape(sequence_blocks.shape[0], -1)
    return jnp.dot(placing, flat_blocks, preferred_element_type=jnp.float32).astype(jnp.bfloat16)


def on_device(
    pool_inputs,
    pool_targets,
    frozen,
    gain,
    adapter_down,
    adapter_up,
    sample_ids,
    buckets,
    lengths,
    destinations,
    competence,
):
    trainers = lax.axis_size("dp")
    sampled = sample_ids.shape[0]
    pool_rows, block_len, feature_part = pool_inputs.shape
    model_width = frozen.shape[0]
    per_pair = max(2, 3 * sampled // (2 * trainers))
    block_capacity = trainers * per_pair
    choosing = sample_ids[:, None] == jnp.arange(pool_rows, dtype=jnp.int32)[None, :]
    chosen_buckets = jnp.sum(jnp.where(choosing, buckets[None, :], 0), axis=1)
    chosen_lengths = jnp.sum(jnp.where(choosing, lengths[None, :], 0), axis=1)
    chosen_inputs = jnp.take(pool_inputs, sample_ids, axis=0)
    chosen_targets = jnp.take(pool_targets, sample_ids, axis=0)
    bucket_range = jnp.arange(NB, dtype=jnp.int32)
    all_buckets, all_lengths = (
        lax.all_gather(chosen_buckets, "dp", axis=0, tiled=True),
        lax.all_gather(chosen_lengths, "dp", axis=0, tiled=True),
    )
    table_onehot = (all_buckets[:, None] == bucket_range[None, :]).astype(jnp.float32)
    counts = jnp.sum(table_onehot * all_lengths[:, None].astype(jnp.float32), axis=0)
    floor_counts = jnp.maximum(counts, 1.0)
    weights = jax.nn.sigmoid(
        SHARPNESS * (competence[0] - (bucket_range.astype(jnp.float32) + 0.5) / NB)
    )
    target_trainer = destinations[:, 0]
    same_dest = target_trainer[:, None] == target_trainer[None, :]
    earlier = jnp.arange(sampled)[None, :] < jnp.arange(sampled)[:, None]
    arrival = jnp.sum((same_dest & earlier).astype(jnp.int32), axis=1)
    slot_index = target_trainer * per_pair + arrival
    slot_match = jnp.arange(block_capacity, dtype=jnp.int32)[:, None] == slot_index[None, :]
    placing = slot_match.astype(jnp.bfloat16)
    slot_bucket = jnp.sum(jnp.where(slot_match, chosen_buckets[None, :], 0), axis=1)
    slot_length = jnp.sum(jnp.where(slot_match, chosen_lengths[None, :], 0), axis=1)
    slot_info = jnp.stack([slot_bucket, slot_length], axis=1)
    send_inputs = place_blocks(placing, chosen_inputs)
    send_targets = place_blocks(placing, chosen_targets)
    got_inputs, got_targets, got_info = (
        lax.all_to_all(send_inputs, "dp", split_axis=0, concat_axis=0, tiled=True),
        lax.all_to_all(send_targets, "dp", split_axis=0, concat_axis=0, tiled=True),
        lax.all_to_all(slot_info, "dp", split_axis=0, concat_axis=0, tiled=True),
    )
    values = got_inputs.reshape(block_capacity * block_len, feature_part).astype(jnp.float32)
    normed = normalize(values, gain, model_width)
    base_gap = frozen_gap(
        values, normed, got_targets.reshape(block_capacity * block_len, feature_part), frozen
    )
    slot_onehot = (got_info[:, 0][:, None] == bucket_range[None, :]).astype(jnp.float32)
    live_mask = (
        (jnp.arange(block_len, dtype=jnp.int32)[None, :] < got_info[:, 1][:, None])
        .astype(jnp.float32)
        .reshape(-1)
    )
    block_coefficient = jnp.sum(slot_onehot * (weights / floor_counts)[None, :], axis=1)
    row_coefficient = jnp.repeat(block_coefficient, block_len)
    down_map = adapter_down[0]
    up_map = adapter_up[0]
    contract_last = (((1,), (1,)), ((), ()))
    contract_first = (((0,), (0,)), ((), ()))
    latent_part = lax.dot_general(
        normed, down_map, contract_last, preferred_element_type=jnp.float32
    )
    latent_rows = lax.psum(latent_part, "mp")
    lowered_rows = (ADAPTER_SCALING * latent_rows).astype(jnp.bfloat16)
    distance = base_gap.astype(jnp.float32) + jnp.dot(
        lowered_rows, up_map, preferred_element_type=jnp.float32
    )
    output_grad = ((2.0 * row_coefficient * live_mask)[:, None] * distance).astype(jnp.bfloat16)
    back_part = lax.dot_general(
        output_grad, up_map, contract_last, preferred_element_type=jnp.float32
    )
    latent_gradient = lax.psum(back_part, "mp")
    lowered_gradient = (ADAPTER_SCALING * latent_gradient).astype(jnp.bfloat16)
    up_gradient = lax.dot_general(
        lowered_rows, output_grad, contract_first, preferred_element_type=jnp.float32
    )
    down_gradient = lax.dot_general(
        lowered_gradient, normed, contract_first, preferred_element_type=jnp.float32
    )
    block_square = jnp.sum(
        (jnp.sum(distance * distance, axis=1) * live_mask).reshape(block_capacity, block_len),
        axis=1,
    )
    partial_value = jnp.sum(slot_onehot * block_square[:, None], axis=0)
    loss_sum = lax.psum(partial_value, ("dp", "mp"))
    bucket_loss = loss_sum / (floor_counts * model_width)
    progress = jnp.sum(weights * bucket_loss) / jnp.sum(bucket_loss)
    competence_next = competence + 0.5 * (1.0 - competence) * progress
    return (down_gradient[None], up_gradient[None], bucket_loss, competence_next)


CONTRACT_LAST = (((1,), (1,)), ((), ()))
CONTRACT_FIRST = (((0,), (0,)), ((), ()))
LANES = 128
CHUNKS = 4


def fused_kernel(
    ids_ref, dest_ref, bucket_ref, length_ref, comp_ref, gain_ref, x_ref, t_ref, frozen_ref, down_ref, up_ref,
    gd_ref, gu_ref, loss_ref, next_ref,
    frozen_buf, x_full, n_full, gain_full, adapters, counts_buf, loss_mp, loss_dp,
    m_dest, m_coef, m_live, m_bucket, gap, spread, grad_out, lat_own, lat_pair, lat_send, lat_recv,
    grads, x_out, x_in, z_out, z_up, z_down,
    local_sem, xs_sem, xr_sem, gain_s, gain_r, au_s, au_r, ad_s, ad_r, ax_s, ax_r, cnt_s, cnt_r,
    lm_s, lm_r, ld_s, ld_r, l1_s, l1_r, l2_s, l2_r, gx_s, gx_r, gu_s, gu_r, gdn_s, gdn_r,
):
    n_dp, n_mp = lax.axis_size("dp"), lax.axis_size("mp")
    d, m = lax.axis_index("dp"), lax.axis_index("mp")
    levels = n_dp // 2
    z, xx = d // 2, d % 2
    tokens, part = x_ref.shape
    rank = down_ref.shape[1]
    blocks = ids_ref.shape[0]
    block_len = tokens // blocks
    groups = n_dp * rank // LANES
    per_group = LANES // rank
    width = n_mp * part
    chunk = tokens // CHUNKS
    half = tokens // 2
    y, core = m // 2, m % 2
    partner, across = y * 2 + (1 - core), (1 - y) * 2 + core
    diagonal = (1 - y) * 2 + (1 - core)
    x_peer = z * 2 + (1 - xx)
    f32, bf16 = jnp.float32, jnp.bfloat16
    pending = []

    def remote(src, dst, s_sem, r_sem, to):
        return pltpu.make_async_remote_copy(
            src_ref=src, dst_ref=dst, send_sem=s_sem, recv_sem=r_sem,
            device_id=to, device_id_type=pl.DeviceIdType.MESH,
        )

    def send(make, when=None):
        if when is None:
            make().start()
        else:
            pl.when(when)(lambda: make().start())
        pending.append((make, when))

    barrier = pltpu.get_barrier_semaphore()
    for j in range(1, n_dp):
        pl.semaphore_signal(barrier, inc=1, device_id=((d + j) % n_dp, m), device_id_type=pl.DeviceIdType.MESH)
    for j in range(1, n_mp):
        pl.semaphore_signal(barrier, inc=1, device_id=(d, (m + j) % n_mp), device_id_type=pl.DeviceIdType.MESH)
    own_down = pltpu.make_async_copy(down_ref.at[0], adapters.at[0, d], local_sem.at[0])
    own_up = pltpu.make_async_copy(up_ref.at[0], adapters.at[1, d], local_sem.at[1])
    own_x = pltpu.make_async_copy(x_ref, x_full.at[m], local_sem.at[2])
    own_frozen = pltpu.make_async_copy(frozen_ref, frozen_buf, local_sem.at[3])
    own_down.start()
    own_up.start()
    own_x.start()
    pl.semaphore_wait(barrier, n_dp - 1 + n_mp - 1)

    def x_copy(kind, i):
        rows = pl.ds(i * chunk, chunk)
        if kind == 0:
            return remote(x_ref.at[rows], x_full.at[m, rows], xs_sem.at[0, i], xr_sem.at[0, i], (d, across))
        if kind == 1:
            return remote(x_ref.at[rows], x_full.at[m, rows], xs_sem.at[1, i], xr_sem.at[1, i], (d, partner))
        return remote(
            x_full.at[across, rows], x_full.at[across, rows], xs_sem.at[2, i], xr_sem.at[2, i], (d, partner)
        )

    def x_wait(kind, i):
        rows = pl.ds(i * chunk, chunk)
        slot = (across, partner, diagonal)[kind]
        view = x_full.at[slot, rows]
        remote(view, view, xs_sem.at[kind, i], xr_sem.at[kind, i], (d, partner)).wait_recv()

    for i in range(CHUNKS):
        send(functools.partial(x_copy, 0, i))
    own_down.wait()
    own_up.wait()

    def a_copy(kind, zt, to):
        s_sem, r_sem = ((au_s, au_r), (ad_s, ad_r), (ax_s, ax_r))[kind]
        view = adapters.at[:, zt * 2 + xx]
        return remote(view, view, s_sem.at[zt], r_sem.at[zt], (to, m))

    def a_wait(kind, zt, slot):
        s_sem, r_sem = ((au_s, au_r), (ad_s, ad_r), (ax_s, ax_r))[kind]
        view = adapters.at[:, slot]
        remote(view, view, s_sem.at[zt], r_sem.at[zt], (x_peer, m)).wait_recv()

    send(lambda: a_copy(2, z, x_peer))
    send(lambda: a_copy(0, z, d + 2), z < levels - 1)
    send(lambda: a_copy(1, z, d - 2), z > 0)
    for i in range(CHUNKS):
        send(functools.partial(x_copy, 1, i))
    gain_full[m] = gain_ref[...]
    for j in range(1, n_mp):
        send(
            lambda j=j: remote(
                gain_ref, gain_full.at[m], gain_s.at[j], gain_r.at[j], (d, (m + j) % n_mp)
            )
        )
    own_frozen.start()

    lane = lax.broadcasted_iota(jnp.int32, (tokens, LANES), 1)
    row = lax.broadcasted_iota(jnp.int32, (tokens, LANES), 0)
    lane64 = lax.broadcasted_iota(jnp.int32, (blocks, LANES), 1)
    named = jnp.where(lane64 < LANES // 2, ids_ref[...], dest_ref[...]).astype(f32).astype(bf16)
    spread_rows = (
        lax.broadcasted_iota(jnp.int32, (tokens, blocks), 0) // block_len
        == lax.broadcasted_iota(jnp.int32, (tokens, blocks), 1)
    ).astype(f32).astype(bf16)
    per_token = jnp.dot(spread_rows, named, preferred_element_type=f32)
    token_id, token_dest = per_token[:, 0:1], per_token[:, LANES // 2:LANES // 2 + 1]
    chosen = token_id == lane.astype(f32)
    token_bucket = jnp.sum(jnp.where(chosen, bucket_ref[...].astype(f32), 0.0), axis=1, keepdims=True)
    token_length = jnp.sum(jnp.where(chosen, length_ref[...].astype(f32), 0.0), axis=1, keepdims=True)
    live = ((row % block_len).astype(f32) < token_length).astype(f32)
    bucket_hot = (token_bucket == lane.astype(f32)).astype(f32)
    m_dest[...] = jnp.broadcast_to(token_dest, (tokens, LANES))
    m_live[...] = live
    m_bucket[...] = bucket_hot
    counts_buf[d] = jnp.broadcast_to(jnp.sum(bucket_hot * live, axis=0, keepdims=True), (8, LANES))

    def spread_tile(buf, s_sem, r_sem, axis):
        count, me = (n_dp, d) if axis == "dp" else (n_mp, m)
        for j in range(1, count):
            to = (me + j) % count
            target = (to, m) if axis == "dp" else (d, to)
            send(lambda j=j, target=target: remote(buf.at[me], buf.at[me], s_sem.at[j], r_sem.at[j], target))

    def gather_tile(buf, s_sem, r_sem, axis):
        count, me = (n_dp, d) if axis == "dp" else (n_mp, m)
        for j in range(1, count):
            source = (me + count - j) % count
            target = (source, m) if axis == "dp" else (d, source)
            remote(buf.at[source], buf.at[source], s_sem.at[j], r_sem.at[j], target).wait_recv()

    own_x.wait()
    for j in range(1, n_mp):
        source = (m + n_mp - j) % n_mp
        remote(gain_ref, gain_full.at[source], gain_s.at[j], gain_r.at[j], (d, source)).wait_recv()
    spread_tile(counts_buf, cnt_s, cnt_r, "dp")

    def normalise(i):
        step = 32

        def body(g, carry):
            rows = pl.ds(pl.multiple_of(i * chunk + g * step, step), step)
            total = jnp.zeros((step, 1), f32)
            for k in range(n_mp):
                v = x_full[k, rows, :].astype(f32)
                total = total + jnp.sum(v * v, axis=1, keepdims=True)
            inverse = lax.rsqrt(total / width + RMS_EPSILON)
            for k in range(n_mp):
                v = x_full[k, rows, :].astype(f32)
                n_full[k, rows, :] = (v * inverse * gain_full[k]).astype(bf16)
            return carry

        lax.fori_loop(0, chunk // step, body, 0)

    def project(h):
        rows = pl.ds(h * half, half)
        tile = 256

        def body(n, carry):
            cols = pl.ds(pl.multiple_of(n * tile, tile), tile)
            acc = jnp.zeros((half, tile), f32)
            for k in range(n_mp):
                acc = acc + jnp.dot(
                    n_full[k, rows, :], frozen_buf[pl.ds(k * part, part), cols], preferred_element_type=f32
                )
            gap[rows, cols] = (
                x_ref[rows, cols].astype(f32) + acc - t_ref[rows, cols].astype(f32)
            ).astype(bf16)
            return carry

        lax.fori_loop(0, part // tile, body, 0)

    def relay(s):
        @pl.when(z - s >= 0)
        def _():
            a_wait(0, z - s, (z - s) * 2 + xx)
        send(lambda: a_copy(2, z - s, x_peer), z - s >= 0)
        send(lambda: a_copy(0, z - s, d + 2), (z - s >= 0) & (z < levels - 1))

        @pl.when(z + s < levels)
        def _():
            a_wait(1, z + s, (z + s) * 2 + xx)
        send(lambda: a_copy(2, z + s, x_peer), z + s < levels)
        send(lambda: a_copy(1, z + s, d - 2), (z + s < levels) & (z > 0))

    for i in range(CHUNKS):
        x_wait(0, i)
        send(functools.partial(x_copy, 2, i))
        if 1 <= i < levels:
            relay(i)
        x_wait(1, i)
        x_wait(2, i)
        normalise(i)
        if i == CHUNKS // 2 - 1:
            own_frozen.wait()
            project(0)
    for s in range(CHUNKS, levels):
        relay(s)
    for zt in range(levels):
        a_wait(2, zt, zt * 2 + (1 - xx))

    tile_rows = 128

    def mask_of(rows, g):
        who = lax.broadcasted_iota(jnp.int32, (tile_rows, LANES), 1) // rank + g * per_group
        return who.astype(f32) == m_dest[rows, :]

    def select(full, rows):
        out = jnp.zeros((tile_rows, LANES), f32)
        for g in range(groups):
            out = out + jnp.where(mask_of(rows, g), full[:, g * LANES:(g + 1) * LANES], 0.0)
        return out

    def over_tiles(body):
        def run(i, carry):
            body(pl.ds(pl.multiple_of(i * tile_rows, tile_rows), tile_rows))
            return carry

        lax.fori_loop(0, tokens // tile_rows, run, 0)

    def stack(which):
        return adapters[which].reshape(n_dp * rank, part)

    def first_half_sum(which):
        send(
            lambda: remote(
                lat_own.at[which], lat_pair.at[which], l1_s.at[which], l1_r.at[which], (d, partner)
            )
        )

    def second_half_sum(which):
        remote(
            lat_own.at[which], lat_pair.at[which], l1_s.at[which], l1_r.at[which], (d, partner)
        ).wait_recv()
        lat_send[which] = (lat_own[which] + lat_pair[which]).astype(bf16)
        send(
            lambda: remote(
                lat_send.at[which], lat_recv.at[which], l2_s.at[which], l2_r.at[which], (d, across)
            )
        )

    def finish_sum(which):
        remote(
            lat_send.at[which], lat_recv.at[which], l2_s.at[which], l2_r.at[which], (d, across)
        ).wait_recv()

        def body(rows):
            total = lat_own[which, rows, :] + lat_pair[which, rows, :] + lat_recv[which, rows, :].astype(f32)
            low = ADAPTER_SCALING * total
            for g in range(groups):
                spread[which, rows, g * LANES:(g + 1) * LANES] = jnp.where(mask_of(rows, g), low, 0.0).astype(bf16)

        over_tiles(body)

    def latent_body(rows):
        full = lax.dot_general(n_full[m, rows, :], stack(0), CONTRACT_LAST, preferred_element_type=f32)
        lat_own[0, rows, :] = select(full, rows)

    over_tiles(latent_body)
    first_half_sum(0)
    gather_tile(counts_buf, cnt_s, cnt_r, "dp")
    counts = counts_buf[0]
    for k in range(1, n_dp):
        counts = counts + counts_buf[k]
    floor_counts = jnp.maximum(counts, 1.0)
    bucket_lane = lax.broadcasted_iota(jnp.int32, (8, LANES), 1)
    competence = comp_ref[...]
    weights = jax.nn.sigmoid(SHARPNESS * (competence - (bucket_lane.astype(f32) + 0.5) / NB))
    rate = jnp.where(bucket_lane < NB, weights / floor_counts, 0.0)[0:1]
    coef = jnp.sum(m_bucket[...] * rate, axis=1, keepdims=True)
    m_coef[...] = 2.0 * coef * m_live[...]
    second_half_sum(0)
    project(1)
    finish_sum(0)

    loss_mp[m] = jnp.zeros((8, LANES), f32)

    def distance_body(rows):
        delta = jnp.dot(spread[0, rows, :], stack(1), preferred_element_type=f32)
        distance = gap[rows, :].astype(f32) + delta
        square = jnp.sum(distance * distance, axis=1, keepdims=True)
        loss_mp[m] += jnp.broadcast_to(
            jnp.sum(m_bucket[rows, :] * (square * m_live[rows, :]), axis=0, keepdims=True), (8, LANES)
        )
        og = (m_coef[rows, 0:1] * distance).astype(bf16)
        grad_out[rows, :] = og
        back = lax.dot_general(og, stack(1), CONTRACT_LAST, preferred_element_type=f32)
        lat_own[1, rows, :] = select(back, rows)

    over_tiles(distance_body)
    first_half_sum(1)

    def gradient(h, values):
        tile = 256

        def body(n, carry):
            cols = pl.ds(pl.multiple_of(n * tile, tile), tile)
            out = lax.dot_general(spread[1 - h, :, :], values(cols), CONTRACT_FIRST, preferred_element_type=f32)
            grads[h, :, :, cols] = out.reshape(n_dp, rank, tile)
            return carry

        lax.fori_loop(0, part // tile, body, 0)
        for p in range(levels):
            if p == levels - 1:
                zt = z
            else:
                falling = levels - 1 - p
                falling = jnp.where(falling > z, falling, falling - 1)
                rising = jnp.where(p < z, p, p + 1)
                zt = jnp.where(z < levels // 2, falling, rising)
            x_out[h, zt] = grads[h, zt * 2 + (1 - xx)].astype(bf16)
            send(
                lambda zt=zt: remote(
                    x_out.at[h, zt], x_in.at[h, zt], gx_s.at[h, zt], gx_r.at[h, zt], (x_peer, m)
                )
            )

    gradient(1, lambda cols: grad_out[:, cols])
    second_half_sum(1)
    spread_tile(loss_mp, lm_s, lm_r, "mp")
    finish_sum(1)
    gradient(0, lambda cols: n_full[m, :, cols])

    gather_tile(loss_mp, lm_s, lm_r, "mp")
    total = loss_mp[0]
    for k in range(1, n_mp):
        total = total + loss_mp[k]
    loss_dp[d] = total

    def arrived(buf, h, zt, s_sem, r_sem):
        view = buf.at[h, zt]
        remote(view, view, s_sem.at[h, zt], r_sem.at[h, zt], (x_peer, m)).wait_recv()
        grads[h, zt * 2 + xx] += buf[h, zt].astype(f32)

    def pass_on(h, s):
        def upward():
            zt = z + s
            arrived(x_in, h, zt, gx_s, gx_r)
            pl.when(z > 0)(lambda: arrived(z_up, h, zt, gu_s, gu_r))
            z_out[h, zt] = grads[h, zt * 2 + xx].astype(bf16)

        def downward():
            zt = z - s
            arrived(x_in, h, zt, gx_s, gx_r)
            pl.when(z < levels - 1)(lambda: arrived(z_down, h, zt, gdn_s, gdn_r))
            z_out[h, zt] = grads[h, zt * 2 + xx].astype(bf16)

        pl.when(z + s < levels)(upward)
        send(
            lambda: remote(
                z_out.at[h, z + s], z_up.at[h, z + s], gu_s.at[h, z + s], gu_r.at[h, z + s], (d + 2, m)
            ),
            z + s < levels,
        )
        pl.when(z - s >= 0)(downward)
        send(
            lambda: remote(
                z_out.at[h, z - s], z_down.at[h, z - s], gdn_s.at[h, z - s], gdn_r.at[h, z - s], (d - 2, m)
            ),
            z - s >= 0,
        )

    spread_tile(loss_dp, ld_s, ld_r, "dp")
    for h, out_ref in ((1, gu_ref), (0, gd_ref)):
        for s in range(levels - 1, 0, -1):
            pass_on(h, s)
        arrived(x_in, h, z, gx_s, gx_r)
        pl.when(z > 0)(lambda h=h: arrived(z_up, h, z, gu_s, gu_r))
        pl.when(z < levels - 1)(lambda h=h: arrived(z_down, h, z, gdn_s, gdn_r))
        out_ref[0] = grads[h, d]

    gather_tile(loss_dp, ld_s, ld_r, "dp")
    loss_sum = loss_dp[0]
    for k in range(1, n_dp):
        loss_sum = loss_sum + loss_dp[k]
    bucket_loss = jnp.where(bucket_lane < NB, loss_sum / (floor_counts * width), 0.0)
    progress = jnp.sum(weights * bucket_loss, axis=1, keepdims=True) / jnp.sum(bucket_loss, axis=1, keepdims=True)
    loss_ref[...] = bucket_loss[0:1]
    next_ref[...] = (competence + 0.5 * (1.0 - competence) * jnp.broadcast_to(progress, (8, LANES)))[0:1]

    for make, when in pending:
        if when is None:
            make().wait_send()
        else:
            pl.when(when)(lambda make=make: make().wait_send())


def on_device_fused(
    pool_inputs, pool_targets, frozen, gain, adapter_down, adapter_up, sample_ids, buckets, lengths, destinations,
    competence,
):
    n_dp, n_mp = lax.axis_size("dp"), lax.axis_size("mp")
    blocks = sample_ids.shape[0]
    pool, block_len, part = pool_inputs.shape
    rank = adapter_down.shape[1]
    tokens = blocks * block_len
    levels = n_dp // 2
    x = pool_inputs.at[sample_ids].get(mode="promise_in_bounds").reshape(tokens, part)
    t = pool_targets.at[sample_ids].get(mode="promise_in_bounds").reshape(tokens, part)
    f32, bf16 = jnp.float32, jnp.bfloat16
    vmem = pl.BlockSpec(memory_space=pltpu.VMEM)
    dma = pltpu.SemaphoreType.DMA
    out = pl.pallas_call(
        fused_kernel,
        out_shape=(
            jax.ShapeDtypeStruct((1, rank, part), f32),
            jax.ShapeDtypeStruct((1, rank, part), f32),
            jax.ShapeDtypeStruct((1, LANES), f32),
            jax.ShapeDtypeStruct((1, LANES), f32),
        ),
        in_specs=[vmem] * 8 + [pl.BlockSpec(memory_space=pl.ANY)] + [vmem] * 2,
        out_specs=(vmem,) * 4,
        scratch_shapes=[
            pltpu.VMEM(frozen.shape, bf16),
            pltpu.VMEM((n_mp, tokens, part), bf16),
            pltpu.VMEM((n_mp, tokens, part), bf16),
            pltpu.VMEM((n_mp, 1, part), f32),
            pltpu.VMEM((2, n_dp, rank, part), bf16),
            pltpu.VMEM((n_dp, 8, LANES), f32),
            pltpu.VMEM((n_mp, 8, LANES), f32),
            pltpu.VMEM((n_dp, 8, LANES), f32),
            pltpu.VMEM((tokens, LANES), f32),
            pltpu.VMEM((tokens, LANES), f32),
            pltpu.VMEM((tokens, LANES), f32),
            pltpu.VMEM((tokens, LANES), f32),
            pltpu.VMEM((tokens, part), bf16),
            pltpu.VMEM((2, tokens, n_dp * rank), bf16),
            pltpu.VMEM((tokens, part), bf16),
            pltpu.VMEM((2, tokens, LANES), f32),
            pltpu.VMEM((2, tokens, LANES), f32),
            pltpu.VMEM((2, tokens, LANES), bf16),
            pltpu.VMEM((2, tokens, LANES), bf16),
            pltpu.VMEM((2, n_dp, rank, part), f32),
            pltpu.VMEM((2, levels, rank, part), bf16),
            pltpu.VMEM((2, levels, rank, part), bf16),
            pltpu.VMEM((2, levels, rank, part), bf16),
            pltpu.VMEM((2, levels, rank, part), bf16),
            pltpu.VMEM((2, levels, rank, part), bf16),
            dma((4,)), dma((3, CHUNKS)), dma((3, CHUNKS)), dma((n_mp,)), dma((n_mp,)),
            dma((levels,)), dma((levels,)), dma((levels,)), dma((levels,)), dma((levels,)), dma((levels,)),
            dma((n_dp,)), dma((n_dp,)), dma((n_mp,)), dma((n_mp,)), dma((n_dp,)), dma((n_dp,)),
            dma((2,)), dma((2,)), dma((2,)), dma((2,)),
            dma((2, levels)), dma((2, levels)), dma((2, levels)), dma((2, levels)), dma((2, levels)), dma((2, levels)),
        ],
        compiler_params=pltpu.CompilerParams(
            collective_id=0, has_side_effects=True, vmem_limit_bytes=58 * 2**20
        ),
        name="fused_step",
    )(
        sample_ids[:, None], destinations, buckets[None, :], lengths[None, :], competence[:, None], gain[None, :],
        x, t, frozen, adapter_down, adapter_up,
    )
    return out[0], out[1], out[2][0, :NB], out[3][0, :1]


def solution(mesh):
    def pick(*args):
        pool_inputs, frozen, adapter_down, sample_ids = args[0], args[2], args[4], args[6]
        tokens, part = sample_ids.shape[0] * pool_inputs.shape[1], pool_inputs.shape[2]
        n_dp, n_mp, rank = lax.axis_size("dp"), lax.axis_size("mp"), adapter_down.shape[1]
        held = 2 * frozen.size + 4 * n_mp * tokens * part + (26 * n_dp + 16) * rank * part
        fits = held < 44 * 2**20 and n_mp == 4 and n_dp % 2 == 0 and n_dp > 2
        exact = pool_inputs.shape[0] == LANES and n_dp * rank % LANES == 0 and LANES % rank == 0
        return (on_device_fused if fits and exact else on_device)(*args)

    in_specs = (
        P("dp", None, "mp"),
        P("dp", None, "mp"),
        P(None, "mp"),
        P("mp"),
        P("dp", None, "mp"),
        P("dp", None, "mp"),
        P("dp"),
        P("dp"),
        P("dp"),
        P("dp", None),
        P(),
    )
    out_specs = (P("dp", None, "mp"), P("dp", None, "mp"), P(), P())
    return jax.shard_map(
        pick, mesh=mesh, in_specs=in_specs, out_specs=out_specs, check_vma=False
    )
```

```python
import functools

import jax
import jax.numpy as jnp
from jax import lax
from jax.experimental import pallas as pl
from jax.experimental.pallas import tpu as pltpu
from jax.sharding import PartitionSpec as P

NB = 16


RMS_EPSILON = 1e-05
SHARPNESS = 12.0
ADAPTER_SCALING = 2.0


def normalize(values, gain, model_width):
    partial_value = jnp.sum(values * values, axis=1)
    square_total = lax.psum(partial_value, "mp")
    inverse_rms = lax.rsqrt(square_total / model_width + RMS_EPSILON)
    return (values * inverse_rms[:, None] * gain[None, :]).astype(jnp.bfloat16)


def frozen_gap(values, normed, targets, frozen):
    projected = jnp.dot(
        lax.all_gather(normed, "mp", axis=1, tiled=True), frozen, preferred_element_type=jnp.float32
    )
    return (values + projected - targets.astype(jnp.float32)).astype(jnp.bfloat16)


def place_blocks(placing, sequence_blocks):
    flat_blocks = sequence_blocks.reshape(sequence_blocks.shape[0], -1)
    return jnp.dot(placing, flat_blocks, preferred_element_type=jnp.float32).astype(jnp.bfloat16)


def on_device(
    pool_inputs,
    pool_targets,
    frozen,
    gain,
    adapter_down,
    adapter_up,
    sample_ids,
    buckets,
    lengths,
    destinations,
    competence,
):
    trainers = lax.axis_size("dp")
    sampled = sample_ids.shape[0]
    pool_rows, block_len, feature_part = pool_inputs.shape
    model_width = frozen.shape[0]
    per_pair = max(2, 3 * sampled // (2 * trainers))
    block_capacity = trainers * per_pair
    choosing = sample_ids[:, None] == jnp.arange(pool_rows, dtype=jnp.int32)[None, :]
    chosen_buckets = jnp.sum(jnp.where(choosing, buckets[None, :], 0), axis=1)
    chosen_lengths = jnp.sum(jnp.where(choosing, lengths[None, :], 0), axis=1)
    chosen_inputs = jnp.take(pool_inputs, sample_ids, axis=0)
    chosen_targets = jnp.take(pool_targets, sample_ids, axis=0)
    bucket_range = jnp.arange(NB, dtype=jnp.int32)
    all_buckets, all_lengths = (
        lax.all_gather(chosen_buckets, "dp", axis=0, tiled=True),
        lax.all_gather(chosen_lengths, "dp", axis=0, tiled=True),
    )
    table_onehot = (all_buckets[:, None] == bucket_range[None, :]).astype(jnp.float32)
    counts = jnp.sum(table_onehot * all_lengths[:, None].astype(jnp.float32), axis=0)
    floor_counts = jnp.maximum(counts, 1.0)
    weights = jax.nn.sigmoid(
        SHARPNESS * (competence[0] - (bucket_range.astype(jnp.float32) + 0.5) / NB)
    )
    target_trainer = destinations[:, 0]
    same_dest = target_trainer[:, None] == target_trainer[None, :]
    earlier = jnp.arange(sampled)[None, :] < jnp.arange(sampled)[:, None]
    arrival = jnp.sum((same_dest & earlier).astype(jnp.int32), axis=1)
    slot_index = target_trainer * per_pair + arrival
    slot_match = jnp.arange(block_capacity, dtype=jnp.int32)[:, None] == slot_index[None, :]
    placing = slot_match.astype(jnp.bfloat16)
    slot_bucket = jnp.sum(jnp.where(slot_match, chosen_buckets[None, :], 0), axis=1)
    slot_length = jnp.sum(jnp.where(slot_match, chosen_lengths[None, :], 0), axis=1)
    slot_info = jnp.stack([slot_bucket, slot_length], axis=1)
    send_inputs = place_blocks(placing, chosen_inputs)
    send_targets = place_blocks(placing, chosen_targets)
    got_inputs, got_targets, got_info = (
        lax.all_to_all(send_inputs, "dp", split_axis=0, concat_axis=0, tiled=True),
        lax.all_to_all(send_targets, "dp", split_axis=0, concat_axis=0, tiled=True),
        lax.all_to_all(slot_info, "dp", split_axis=0, concat_axis=0, tiled=True),
    )
    values = got_inputs.reshape(block_capacity * block_len, feature_part).astype(jnp.float32)
    normed = normalize(values, gain, model_width)
    base_gap = frozen_gap(
        values, normed, got_targets.reshape(block_capacity * block_len, feature_part), frozen
    )
    slot_onehot = (got_info[:, 0][:, None] == bucket_range[None, :]).astype(jnp.float32)
    live_mask = (
        (jnp.arange(block_len, dtype=jnp.int32)[None, :] < got_info[:, 1][:, None])
        .astype(jnp.float32)
        .reshape(-1)
    )
    block_coefficient = jnp.sum(slot_onehot * (weights / floor_counts)[None, :], axis=1)
    row_coefficient = jnp.repeat(block_coefficient, block_len)
    down_map = adapter_down[0]
    up_map = adapter_up[0]
    contract_last = (((1,), (1,)), ((), ()))
    contract_first = (((0,), (0,)), ((), ()))
    latent_part = lax.dot_general(
        normed, down_map, contract_last, preferred_element_type=jnp.float32
    )
    latent_rows = lax.psum(latent_part, "mp")
    lowered_rows = (ADAPTER_SCALING * latent_rows).astype(jnp.bfloat16)
    distance = base_gap.astype(jnp.float32) + jnp.dot(
        lowered_rows, up_map, preferred_element_type=jnp.float32
    )
    output_grad = ((2.0 * row_coefficient * live_mask)[:, None] * distance).astype(jnp.bfloat16)
    back_part = lax.dot_general(
        output_grad, up_map, contract_last, preferred_element_type=jnp.float32
    )
    latent_gradient = lax.psum(back_part, "mp")
    lowered_gradient = (ADAPTER_SCALING * latent_gradient).astype(jnp.bfloat16)
    up_gradient = lax.dot_general(
        lowered_rows, output_grad, contract_first, preferred_element_type=jnp.float32
    )
    down_gradient = lax.dot_general(
        lowered_gradient, normed, contract_first, preferred_element_type=jnp.float32
    )
    block_square = jnp.sum(
        (jnp.sum(distance * distance, axis=1) * live_mask).reshape(block_capacity, block_len),
        axis=1,
    )
    partial_value = jnp.sum(slot_onehot * block_square[:, None], axis=0)
    loss_sum = lax.psum(partial_value, ("dp", "mp"))
    bucket_loss = loss_sum / (floor_counts * model_width)
    progress = jnp.sum(weights * bucket_loss) / jnp.sum(bucket_loss)
    competence_next = competence + 0.5 * (1.0 - competence) * progress
    return (down_gradient[None], up_gradient[None], bucket_loss, competence_next)


CONTRACT_LAST = (((1,), (1,)), ((), ()))
CONTRACT_FIRST = (((0,), (0,)), ((), ()))
LANES = 128
CHUNKS = 4


def fused_kernel(
    ids_ref, dest_ref, bucket_ref, length_ref, comp_ref, gain_ref, x_ref, pool_ref, frozen_ref, down_ref, up_ref,
    gd_ref, gu_ref, loss_ref, next_ref,
    frozen_buf, pool_buf, t_ref, x_full, n_full, gain_full, adapters, counts_buf, loss_mp, loss_dp,
    m_dest, m_coef, m_live, m_bucket, gap, spread, grad_out, lat_own, lat_pair, lat_send, lat_recv,
    grads, x_out, x_in, z_out, z_up, z_down, w_out, w_up, w_down,
    local_sem, xs_sem, xr_sem, gain_s, gain_r, au_s, au_r, ad_s, ad_r, ax_s, ax_r, cnt_s, cnt_r,
    lm_s, lm_r, ld_s, ld_r, l1_s, l1_r, l2_s, l2_r, gx_s, gx_r, gu_s, gu_r, gdn_s, gdn_r,
):
    n_dp, n_mp = lax.axis_size("dp"), lax.axis_size("mp")
    d, m = lax.axis_index("dp"), lax.axis_index("mp")
    levels = n_dp // 2
    z, xx = d // 2, d % 2
    tokens, part = x_ref.shape
    rank = down_ref.shape[1]
    blocks = ids_ref.shape[1]
    block_len = tokens // blocks
    groups = n_dp * rank // LANES
    per_group = LANES // rank
    width = n_mp * part
    chunk = tokens // CHUNKS
    half = tokens // 2
    y, core = m // 2, m % 2
    partner, across = y * 2 + (1 - core), (1 - y) * 2 + core
    diagonal = (1 - y) * 2 + (1 - core)
    x_peer = z * 2 + (1 - xx)
    f32, bf16 = jnp.float32, jnp.bfloat16
    pending = []

    def remote(src, dst, s_sem, r_sem, to):
        return pltpu.make_async_remote_copy(
            src_ref=src, dst_ref=dst, send_sem=s_sem, recv_sem=r_sem,
            device_id=to, device_id_type=pl.DeviceIdType.MESH,
        )

    def send(make, when=None):
        if when is None:
            make().start()
        else:
            pl.when(when)(lambda: make().start())
        pending.append((make, when))

    barrier = pltpu.get_barrier_semaphore()
    for j in range(1, n_dp):
        pl.semaphore_signal(barrier, inc=1, device_id=((d + j) % n_dp, m), device_id_type=pl.DeviceIdType.MESH)
    for j in range(1, n_mp):
        pl.semaphore_signal(barrier, inc=1, device_id=(d, (m + j) % n_mp), device_id_type=pl.DeviceIdType.MESH)
    own_down = pltpu.make_async_copy(down_ref.at[0], adapters.at[0, d], local_sem.at[0])
    own_up = pltpu.make_async_copy(up_ref.at[0], adapters.at[1, d], local_sem.at[1])
    own_x = pltpu.make_async_copy(x_ref, x_full.at[m], local_sem.at[2])
    own_frozen = pltpu.make_async_copy(frozen_ref, frozen_buf, local_sem.at[3])
    own_down.start()
    own_up.start()
    own_x.start()
    pl.semaphore_wait(barrier, n_dp - 1 + n_mp - 1)

    def x_copy(kind, i):
        rows = pl.ds(i * chunk, chunk)
        if kind == 0:
            return remote(x_ref.at[rows], x_full.at[m, rows], xs_sem.at[0, i], xr_sem.at[0, i], (d, across))
        if kind == 1:
            return remote(x_ref.at[rows], x_full.at[m, rows], xs_sem.at[1, i], xr_sem.at[1, i], (d, partner))
        return remote(
            x_full.at[across, rows], x_full.at[across, rows], xs_sem.at[2, i], xr_sem.at[2, i], (d, partner)
        )

    def x_wait(kind, i):
        rows = pl.ds(i * chunk, chunk)
        slot = (across, partner, diagonal)[kind]
        view = x_full.at[slot, rows]
        remote(view, view, xs_sem.at[kind, i], xr_sem.at[kind, i], (d, partner)).wait_recv()

    own_down.wait()
    own_up.wait()

    def a_copy(kind, zt, to):
        s_sem, r_sem = ((au_s, au_r), (ad_s, ad_r), (ax_s, ax_r))[kind]
        view = adapters.at[:, zt * 2 + xx]
        return remote(view, view, s_sem.at[zt], r_sem.at[zt], (to, m))

    def a_wait(kind, zt, slot):
        s_sem, r_sem = ((au_s, au_r), (ad_s, ad_r), (ax_s, ax_r))[kind]
        view = adapters.at[:, slot]
        remote(view, view, s_sem.at[zt], r_sem.at[zt], (x_peer, m)).wait_recv()

    send(lambda: a_copy(2, z, x_peer))
    send(lambda: a_copy(0, z, d + 2), z < levels - 1)
    send(lambda: a_copy(1, z, d - 2), z > 0)
    send(functools.partial(x_copy, 0, 0))
    for i in range(CHUNKS):
        send(functools.partial(x_copy, 1, i))
    gain_full[m] = gain_ref[...]
    for j in range(1, n_mp):
        send(
            lambda j=j: remote(
                gain_ref, gain_full.at[m], gain_s.at[j], gain_r.at[j], (d, (m + j) % n_mp)
            )
        )
    own_pool = pltpu.make_async_copy(pool_ref, pool_buf, local_sem.at[4])
    own_pool.start()
    own_frozen.start()

    lane = lax.broadcasted_iota(jnp.int32, (tokens, LANES), 1)
    row = lax.broadcasted_iota(jnp.int32, (tokens, LANES), 0)
    first_row = lax.broadcasted_iota(jnp.int32, (LANES, blocks), 0) < LANES // 2
    named = jnp.where(first_row, ids_ref[...], dest_ref[...]).astype(f32).astype(bf16)
    spread_rows = (
        lax.broadcasted_iota(jnp.int32, (tokens, blocks), 0) // block_len
        == lax.broadcasted_iota(jnp.int32, (tokens, blocks), 1)
    ).astype(f32).astype(bf16)
    per_token = lax.dot_general(spread_rows, named, CONTRACT_LAST, preferred_element_type=f32)
    token_id, token_dest = per_token[:, 0:1], per_token[:, LANES // 2:LANES // 2 + 1]
    chosen = token_id == lane.astype(f32)
    token_bucket = jnp.sum(jnp.where(chosen, bucket_ref[...].astype(f32), 0.0), axis=1, keepdims=True)
    token_length = jnp.sum(jnp.where(chosen, length_ref[...].astype(f32), 0.0), axis=1, keepdims=True)
    live = ((row % block_len).astype(f32) < token_length).astype(f32)
    bucket_hot = (token_bucket == lane.astype(f32)).astype(f32)
    m_dest[...] = jnp.broadcast_to(token_dest, (tokens, LANES))
    m_coef[...] = jnp.broadcast_to(token_id, (tokens, LANES))
    m_live[...] = live
    m_bucket[...] = bucket_hot
    counts_buf[d] = jnp.broadcast_to(jnp.sum(bucket_hot * live, axis=0, keepdims=True), (8, LANES))

    def spread_tile(buf, s_sem, r_sem, axis):
        count, me = (n_dp, d) if axis == "dp" else (n_mp, m)
        for j in range(1, count):
            to = (me + j) % count
            target = (to, m) if axis == "dp" else (d, to)
            send(lambda j=j, target=target: remote(buf.at[me], buf.at[me], s_sem.at[j], r_sem.at[j], target))

    def gather_tile(buf, s_sem, r_sem, axis):
        count, me = (n_dp, d) if axis == "dp" else (n_mp, m)
        for j in range(1, count):
            source = (me + count - j) % count
            target = (source, m) if axis == "dp" else (d, source)
            remote(buf.at[source], buf.at[source], s_sem.at[j], r_sem.at[j], target).wait_recv()

    own_x.wait()
    for j in range(1, n_mp):
        source = (m + n_mp - j) % n_mp
        remote(gain_ref, gain_full.at[source], gain_s.at[j], gain_r.at[j], (d, source)).wait_recv()
    spread_tile(counts_buf, cnt_s, cnt_r, "dp")

    own_pool.wait()

    def pick_targets(i, carry):
        rows = pl.ds(pl.multiple_of(i * 128, 128), 128)
        stored = pool_buf.shape[0]
        pool_row = lax.broadcasted_iota(jnp.int32, (128, stored), 1)
        place = lax.broadcasted_iota(jnp.int32, (128, 1), 0) % block_len
        wanted = m_coef[rows, 0:1] * block_len + place.astype(f32)
        hot = (pool_row.astype(f32) == wanted).astype(f32).astype(bf16)
        t_ref[rows, :] = jnp.dot(hot, pool_buf[...], preferred_element_type=f32).astype(bf16)
        return carry

    lax.fori_loop(0, tokens // 128, pick_targets, 0)

    def normalise(i):
        step = 32

        def body(g, carry):
            rows = pl.ds(pl.multiple_of(i * chunk + g * step, step), step)
            total = jnp.zeros((step, 1), f32)
            for k in range(n_mp):
                v = x_full[k, rows, :].astype(f32)
                total = total + jnp.sum(v * v, axis=1, keepdims=True)
            inverse = lax.rsqrt(total / width + RMS_EPSILON)
            for k in range(n_mp):
                v = x_full[k, rows, :].astype(f32)
                n_full[k, rows, :] = (v * inverse * gain_full[k]).astype(bf16)
            return carry

        lax.fori_loop(0, chunk // step, body, 0)

    def project(h):
        rows = pl.ds(h * half, half)
        tile = 256

        def body(n, carry):
            cols = pl.ds(pl.multiple_of(n * tile, tile), tile)
            acc = jnp.zeros((half, tile), f32)
            for k in range(n_mp):
                acc = acc + jnp.dot(
                    n_full[k, rows, :], frozen_buf[pl.ds(k * part, part), cols], preferred_element_type=f32
                )
            gap[rows, cols] = (
                x_ref[rows, cols].astype(f32) + acc - t_ref[rows, cols].astype(f32)
            ).astype(bf16)
            return carry

        lax.fori_loop(0, part // tile, body, 0)

    def relay(s):
        @pl.when(z - s >= 0)
        def _():
            a_wait(0, z - s, (z - s) * 2 + xx)
        send(lambda: a_copy(2, z - s, x_peer), z - s >= 0)
        send(lambda: a_copy(0, z - s, d + 2), (z - s >= 0) & (z < levels - 1))

        @pl.when(z + s < levels)
        def _():
            a_wait(1, z + s, (z + s) * 2 + xx)
        send(lambda: a_copy(2, z + s, x_peer), z + s < levels)
        send(lambda: a_copy(1, z + s, d - 2), (z + s < levels) & (z > 0))

    for s in range(1, levels):
        relay(s)
        if s < CHUNKS:
            send(functools.partial(x_copy, 0, s))
    for i in range(levels, CHUNKS):
        send(functools.partial(x_copy, 0, i))
    for i in range(CHUNKS):
        x_wait(0, i)
        send(functools.partial(x_copy, 2, i))
        x_wait(1, i)
        x_wait(2, i)
        normalise(i)
        if i == CHUNKS // 2 - 1:
            own_frozen.wait()
            project(0)
    for zt in range(levels):
        a_wait(2, zt, zt * 2 + (1 - xx))

    tile_rows = 128

    def mask_of(rows, g):
        who = lax.broadcasted_iota(jnp.int32, (tile_rows, LANES), 1) // rank + g * per_group
        return who.astype(f32) == m_dest[rows, :]

    def select(full, rows):
        out = jnp.zeros((tile_rows, LANES), f32)
        for g in range(groups):
            out = out + jnp.where(mask_of(rows, g), full[:, g * LANES:(g + 1) * LANES], 0.0)
        return out

    def over_tiles(body):
        def run(i, carry):
            body(pl.ds(pl.multiple_of(i * tile_rows, tile_rows), tile_rows))
            return carry

        lax.fori_loop(0, tokens // tile_rows, run, 0)

    def stack(which):
        return adapters[which].reshape(n_dp * rank, part)

    def first_half_sum(which):
        send(
            lambda: remote(
                lat_own.at[which], lat_pair.at[which], l1_s.at[which], l1_r.at[which], (d, partner)
            )
        )

    def second_half_sum(which):
        remote(
            lat_own.at[which], lat_pair.at[which], l1_s.at[which], l1_r.at[which], (d, partner)
        ).wait_recv()
        lat_send[which] = (lat_own[which] + lat_pair[which]).astype(bf16)
        send(
            lambda: remote(
                lat_send.at[which], lat_recv.at[which], l2_s.at[which], l2_r.at[which], (d, across)
            )
        )

    def finish_sum(which):
        remote(
            lat_send.at[which], lat_recv.at[which], l2_s.at[which], l2_r.at[which], (d, across)
        ).wait_recv()

        def body(rows):
            total = lat_own[which, rows, :] + lat_pair[which, rows, :] + lat_recv[which, rows, :].astype(f32)
            low = ADAPTER_SCALING * total
            for g in range(groups):
                spread[which, rows, g * LANES:(g + 1) * LANES] = jnp.where(mask_of(rows, g), low, 0.0).astype(bf16)

        over_tiles(body)

    def latent_body(rows):
        full = lax.dot_general(n_full[m, rows, :], stack(0), CONTRACT_LAST, preferred_element_type=f32)
        lat_own[0, rows, :] = select(full, rows)

    over_tiles(latent_body)
    first_half_sum(0)
    gather_tile(counts_buf, cnt_s, cnt_r, "dp")
    counts = counts_buf[0]
    for k in range(1, n_dp):
        counts = counts + counts_buf[k]
    floor_counts = jnp.maximum(counts, 1.0)
    bucket_lane = lax.broadcasted_iota(jnp.int32, (8, LANES), 1)
    competence = comp_ref[...]
    weights = jax.nn.sigmoid(SHARPNESS * (competence - (bucket_lane.astype(f32) + 0.5) / NB))
    rate = jnp.where(bucket_lane < NB, weights / floor_counts, 0.0)[0:1]
    coef = jnp.sum(m_bucket[...] * rate, axis=1, keepdims=True)
    m_coef[...] = 2.0 * coef * m_live[...]
    second_half_sum(0)
    project(1)
    finish_sum(0)

    loss_mp[m] = jnp.zeros((8, LANES), f32)

    def distance_body(rows):
        delta = jnp.dot(spread[0, rows, :], stack(1), preferred_element_type=f32)
        distance = gap[rows, :].astype(f32) + delta
        square = jnp.sum(distance * distance, axis=1, keepdims=True)
        loss_mp[m] += jnp.broadcast_to(
            jnp.sum(m_bucket[rows, :] * (square * m_live[rows, :]), axis=0, keepdims=True), (8, LANES)
        )
        og = (m_coef[rows, 0:1] * distance).astype(bf16)
        grad_out[rows, :] = og
        back = lax.dot_general(og, stack(1), CONTRACT_LAST, preferred_element_type=f32)
        lat_own[1, rows, :] = select(back, rows)

    over_tiles(distance_body)
    first_half_sum(1)

    def gradient(h, values):
        tile = 256

        def body(n, carry):
            cols = pl.ds(pl.multiple_of(n * tile, tile), tile)
            out = lax.dot_general(spread[1 - h, :, :], values(cols), CONTRACT_FIRST, preferred_element_type=f32)
            grads[h, :, :, cols] = out.reshape(n_dp, rank, tile)
            return carry

        lax.fori_loop(0, part // tile, body, 0)

    def send_sideways(h, positions):
        for p in positions:
            if p == levels - 1:
                zt = z
            else:
                falling = levels - 1 - p
                falling = jnp.where(falling > z, falling, falling - 1)
                rising = jnp.where(p < z, p, p + 1)
                zt = jnp.where(z < levels // 2, falling, rising)
            x_out[h, zt] = grads[h, zt * 2 + (1 - xx)].astype(bf16)
            send(
                lambda zt=zt: remote(
                    x_out.at[h, zt], x_in.at[h, zt], gx_s.at[h, zt], gx_r.at[h, zt], (x_peer, m)
                )
            )

    gradient(1, lambda cols: grad_out[:, cols])
    second_half_sum(1)
    spread_tile(loss_mp, lm_s, lm_r, "mp")
    send_sideways(1, range(2))
    finish_sum(1)
    gradient(0, lambda cols: n_full[m, :, cols])

    gather_tile(loss_mp, lm_s, lm_r, "mp")
    total = loss_mp[0]
    for k in range(1, n_mp):
        total = total + loss_mp[k]
    loss_dp[d] = total

    def arrived(buf, h, zt, s_sem, r_sem):
        view = buf.at[h, zt]
        remote(view, view, s_sem.at[h, zt], r_sem.at[h, zt], (x_peer, m)).wait_recv()
        grads[h, zt * 2 + xx] += buf[h, zt].astype(f32)

    def came(buf, zt, s_sem, r_sem):
        view = buf.at[zt]
        remote(view, view, s_sem.at[0, zt], r_sem.at[0, zt], (x_peer, m)).wait_recv()
        grads[0, pl.ds(zt * 2, 2)] += buf[zt].astype(f32)

    def pass_pair(s):
        def upward():
            zt = z + s
            pl.when(z > 0)(lambda: came(w_up, zt, gu_s, gu_r))
            w_out[zt] = grads[0, pl.ds(zt * 2, 2)].astype(bf16)

        def downward():
            zt = z - s
            pl.when(z < levels - 1)(lambda: came(w_down, zt, gdn_s, gdn_r))
            w_out[zt] = grads[0, pl.ds(zt * 2, 2)].astype(bf16)

        pl.when(z + s < levels)(upward)
        send(
            lambda: remote(w_out.at[z + s], w_up.at[z + s], gu_s.at[0, z + s], gu_r.at[0, z + s], (d + 2, m)),
            z + s < levels,
        )
        pl.when(z - s >= 0)(downward)
        send(
            lambda: remote(w_out.at[z - s], w_down.at[z - s], gdn_s.at[0, z - s], gdn_r.at[0, z - s], (d - 2, m)),
            z - s >= 0,
        )

    def pass_on(s):
        def upward():
            zt = z + s
            arrived(x_in, 1, zt, gx_s, gx_r)
            pl.when(z > 0)(lambda: arrived(z_up, 1, zt, gu_s, gu_r))
            z_out[1, zt] = grads[1, zt * 2 + xx].astype(bf16)

        def downward():
            zt = z - s
            arrived(x_in, 1, zt, gx_s, gx_r)
            pl.when(z < levels - 1)(lambda: arrived(z_down, 1, zt, gdn_s, gdn_r))
            z_out[1, zt] = grads[1, zt * 2 + xx].astype(bf16)

        pl.when(z + s < levels)(upward)
        send(
            lambda: remote(
                z_out.at[1, z + s], z_up.at[1, z + s], gu_s.at[1, z + s], gu_r.at[1, z + s], (d + 2, m)
            ),
            z + s < levels,
        )
        pl.when(z - s >= 0)(downward)
        send(
            lambda: remote(
                z_out.at[1, z - s], z_down.at[1, z - s], gdn_s.at[1, z - s], gdn_r.at[1, z - s], (d - 2, m)
            ),
            z - s >= 0,
        )

    spread_tile(loss_dp, ld_s, ld_r, "dp")
    for s in range(levels - 1, 0, -1):
        pass_pair(s)
        if levels - s >= 2:
            send_sideways(1, (levels - s,))
        pass_on(s)
    pl.when(z > 0)(lambda: came(w_up, z, gu_s, gu_r))
    pl.when(z < levels - 1)(lambda: came(w_down, z, gdn_s, gdn_r))
    x_out[0, z] = grads[0, z * 2 + (1 - xx)].astype(bf16)
    send(lambda: remote(x_out.at[0, z], x_in.at[0, z], gx_s.at[0, z], gx_r.at[0, z], (x_peer, m)))
    arrived(x_in, 1, z, gx_s, gx_r)
    pl.when(z > 0)(lambda: arrived(z_up, 1, z, gu_s, gu_r))
    pl.when(z < levels - 1)(lambda: arrived(z_down, 1, z, gdn_s, gdn_r))
    gu_ref[0] = grads[1, d]
    arrived(x_in, 0, z, gx_s, gx_r)
    gd_ref[0] = grads[0, d]

    gather_tile(loss_dp, ld_s, ld_r, "dp")
    loss_sum = loss_dp[0]
    for k in range(1, n_dp):
        loss_sum = loss_sum + loss_dp[k]
    bucket_loss = jnp.where(bucket_lane < NB, loss_sum / (floor_counts * width), 0.0)
    progress = jnp.sum(weights * bucket_loss, axis=1, keepdims=True) / jnp.sum(bucket_loss, axis=1, keepdims=True)
    loss_ref[...] = bucket_loss[0:1]
    next_ref[...] = (competence + 0.5 * (1.0 - competence) * jnp.broadcast_to(progress, (8, LANES)))[0:1]

    for make, when in pending:
        if when is None:
            make().wait_send()
        else:
            pl.when(when)(lambda make=make: make().wait_send())


def on_device_fused(
    pool_inputs, pool_targets, frozen, gain, adapter_down, adapter_up, sample_ids, buckets, lengths, destinations,
    competence,
):
    n_dp, n_mp = lax.axis_size("dp"), lax.axis_size("mp")
    blocks = sample_ids.shape[0]
    pool, block_len, part = pool_inputs.shape
    rank = adapter_down.shape[1]
    tokens = blocks * block_len
    levels = n_dp // 2
    x = pool_inputs.at[sample_ids].get(mode="promise_in_bounds", wrap_negative_indices=False).reshape(tokens, part)
    t = pool_targets.reshape(pool * block_len, part)
    f32, bf16 = jnp.float32, jnp.bfloat16
    vmem = pl.BlockSpec(memory_space=pltpu.VMEM)
    dma = pltpu.SemaphoreType.DMA
    out = pl.pallas_call(
        fused_kernel,
        out_shape=(
            jax.ShapeDtypeStruct((1, rank, part), f32),
            jax.ShapeDtypeStruct((1, rank, part), f32),
            jax.ShapeDtypeStruct((1, LANES), f32),
            jax.ShapeDtypeStruct((1, LANES), f32),
        ),
        in_specs=[vmem] * 7 + [pl.BlockSpec(memory_space=pl.ANY)] * 2 + [vmem] * 2,
        out_specs=(vmem,) * 4,
        scratch_shapes=[
            pltpu.VMEM(frozen.shape, bf16),
            pltpu.VMEM(t.shape, bf16),
            pltpu.VMEM((tokens, part), bf16),
            pltpu.VMEM((n_mp, tokens, part), bf16),
            pltpu.VMEM((n_mp, tokens, part), bf16),
            pltpu.VMEM((n_mp, 1, part), f32),
            pltpu.VMEM((2, n_dp, rank, part), bf16),
            pltpu.VMEM((n_dp, 8, LANES), f32),
            pltpu.VMEM((n_mp, 8, LANES), f32),
            pltpu.VMEM((n_dp, 8, LANES), f32),
            pltpu.VMEM((tokens, LANES), f32),
            pltpu.VMEM((tokens, LANES), f32),
            pltpu.VMEM((tokens, LANES), f32),
            pltpu.VMEM((tokens, LANES), f32),
            pltpu.VMEM((tokens, part), bf16),
            pltpu.VMEM((2, tokens, n_dp * rank), bf16),
            pltpu.VMEM((tokens, part), bf16),
            pltpu.VMEM((2, tokens, LANES), f32),
            pltpu.VMEM((2, tokens, LANES), f32),
            pltpu.VMEM((2, tokens, LANES), bf16),
            pltpu.VMEM((2, tokens, LANES), bf16),
            pltpu.VMEM((2, n_dp, rank, part), f32),
            pltpu.VMEM((2, levels, rank, part), bf16),
            pltpu.VMEM((2, levels, rank, part), bf16),
            pltpu.VMEM((2, levels, rank, part), bf16),
            pltpu.VMEM((2, levels, rank, part), bf16),
            pltpu.VMEM((2, levels, rank, part), bf16),
            pltpu.VMEM((levels, 2, rank, part), bf16),
            pltpu.VMEM((levels, 2, rank, part), bf16),
            pltpu.VMEM((levels, 2, rank, part), bf16),
            dma((5,)), dma((3, CHUNKS)), dma((3, CHUNKS)), dma((n_mp,)), dma((n_mp,)),
            dma((levels,)), dma((levels,)), dma((levels,)), dma((levels,)), dma((levels,)), dma((levels,)),
            dma((n_dp,)), dma((n_dp,)), dma((n_mp,)), dma((n_mp,)), dma((n_dp,)), dma((n_dp,)),
            dma((2,)), dma((2,)), dma((2,)), dma((2,)),
            dma((2, levels)), dma((2, levels)), dma((2, levels)), dma((2, levels)), dma((2, levels)), dma((2, levels)),
        ],
        compiler_params=pltpu.CompilerParams(
            collective_id=0, has_side_effects=True, vmem_limit_bytes=58 * 2**20
        ),
        name="fused_step",
    )(
        sample_ids[None, :], destinations.reshape(1, blocks), buckets[None, :], lengths[None, :], competence[:, None], gain[None, :],
        x, t, frozen, adapter_down, adapter_up,
    )
    return out[0], out[1], out[2][0, :NB], out[3][0, :1]


def solution(mesh):
    def pick(*args):
        pool_inputs, frozen, adapter_down, sample_ids = args[0], args[2], args[4], args[6]
        tokens, part = sample_ids.shape[0] * pool_inputs.shape[1], pool_inputs.shape[2]
        n_dp, n_mp, rank = lax.axis_size("dp"), lax.axis_size("mp"), adapter_down.shape[1]
        held = 2 * frozen.size + 4 * n_mp * tokens * part + (32 * n_dp + 16) * rank * part + 2 * pool_inputs.size
        fits = held < 44 * 2**20 and n_mp == 4 and n_dp % 2 == 0 and n_dp > 2
        exact = pool_inputs.shape[0] == LANES and n_dp * rank % LANES == 0 and LANES % rank == 0
        return (on_device_fused if fits and exact else on_device)(*args)

    in_specs = (
        P("dp", None, "mp"),
        P("dp", None, "mp"),
        P(None, "mp"),
        P("mp"),
        P("dp", None, "mp"),
        P("dp", None, "mp"),
        P("dp"),
        P("dp"),
        P("dp"),
        P("dp", None),
        P(),
    )
    out_specs = (P("dp", None, "mp"), P("dp", None, "mp"), P(), P())
    return jax.shard_map(
        pick, mesh=mesh, in_specs=in_specs, out_specs=out_specs, check_vma=False
    )
```
